32 devices in a mesh: sub: 16 (over z, y, x), crs: 2 (over core).
Axes of the slice: x: 2, y: 2, z: 4, core: 2. Of those that a mesh axis runs over, the one named last changes fastest.
Arguments:
- multipliers: float32 [16, 128, 512], P(None, ('sub', 'crs')), may hold values from -6 to 6
- own_modes: float32 [6, 128, 512], P(None, ('sub', 'crs')), may hold values from -0.75 to 0.75
- neighbour_modes: float32 [6, 128, 512], P(None, ('sub', 'crs')), may hold values from -0.75 to 0.75
- face_index: int32 [128, 512], P(('sub', 'crs')), may hold values from 0 to 5, as said below
- neighbour_list: int32 [128, 6], replicated, may hold values from 0 to 127, as said below
- coarse_factor: float32 [768, 768], P('sub', 'crs'), may hold values from -0.21875 to 0.21875
Outputs:
- projected: float32 [16, 128, 512], P(None, ('sub', 'crs'))
The draws below stay inside these ranges and needn't reach their ends.
Inputs may be any that keep to these rules, and one draw needn't show every extreme that they name: `face_index`: the multipliers of each subdomain lie in 6 contiguous nonempty blocks, face 0 first and face 5 last. `neighbour_list`: subdomain s = (8 x + y) * 8 + z sits at (x, y, z) of a periodic grid of 2 x 8 x 8 subdomains; the 6 faces of each subdomain name its grid neighbours x plus 1, x minus 1, y plus or minus 1, z plus or minus 1 (periodic; along the first dimension both name the same subdomain), in an order that differs from subdomain to subdomain.
All inputs are finite; a program needn't handle non-finite values.
Results may differ from the reference program's by a relative error of at most 0.0001.
Values sent between devices are 32-bit elements; how exact they have to be, the bound alone decides.
No kernel may reach another device: no remote copies, remote signals or barrier semaphores. Data moves between devices by JAX's collectives and lax.ppermute only.
A program may use at most 64 MiB of HBM per device.

```python
import jax
import jax.numpy as jnp
from jax import lax

MODES = 6
NFACE = 6
IW = 512
NRHS = 16
NSUB = 128
NC = 768
GY = 8
GX = 2
GZ = 8


def draw_face_index(key, part):
    block = IW // NFACE
    spread = block // 4
    jitter = jax.random.randint(key, (NSUB, NFACE - 1), -spread, spread + 1).astype(jnp.int32)
    starts = (lax.broadcasted_iota(jnp.int32, (NSUB, NFACE - 1), 1) + 1) * block + jitter
    places = lax.broadcasted_iota(jnp.int32, (NSUB, IW), 1)
    passed = (places[:, :, None] >= starts[:, None, :]).astype(jnp.int32)
    return jnp.sum(passed, axis=2).astype(jnp.int32)


def draw_neighbour_list(key, part):
    scores = jax.random.randint(jax.random.fold_in(key, 17), (NSUB, NFACE), 0, 1 << 20).astype(jnp.int32)
    scores = scores * 8 + lax.broadcasted_iota(jnp.int32, (NSUB, NFACE), 1)
    order = jnp.argsort(scores, axis=1, stable=True).astype(jnp.int32)
    cells = lax.iota(jnp.int32, NSUB)
    first = cells // (GY * GZ)
    second = cells // GZ % GY
    third = cells % GZ

    def place(a, b, c):
        return ((a * GY + b) * GZ + c).astype(jnp.int32)
    table = jnp.stack([place((first + 1) % GX, second, third), place((first + GX - 1) % GX, second, third), place(first, (second + 1) % GY, third), place(first, (second + GY - 1) % GY, third), place(first, second, (third + 1) % GZ), place(first, second, (third + GZ - 1) % GZ)], axis=1)
    return jnp.take_along_axis(table, order, axis=1).astype(jnp.int32)


def levels(stream_key, dims, cuts, low, top_value):
    gain = 1.0
    for dim, parts in cuts:
        draws = jax.random.uniform(jax.random.fold_in(jax.random.fold_in(stream_key, 6), dim), (parts,), jnp.float32, low / len(cuts), top_value / len(cuts))
        gain = gain * jnp.repeat(jnp.exp(draws), dims[dim] // parts).reshape((-1,) + (1,) * (len(dims) - 1 - dim))
    return gain


def normal_values(key, shape, scale, most, shards=(), kind=jnp.bfloat16):
    array = jax.random.normal(key, shape, jnp.float32) * scale
    if len(shards) > 0:
        array = levels(key, shape, shards, -0.22, 0.18) * array
    return jnp.clip(array, min=-most, max=most).astype(kind)


def setup_inputs(seed: int = 0) -> dict:
    seeds = jax.random.split(jax.random.key(seed), 7)
    return {
        "multipliers": normal_values(seeds[0], (NRHS, NSUB, IW), 1.0, 6.0, ((1, 32),), jnp.float32),
        "own_modes": normal_values(seeds[1], (MODES, NSUB, IW), (IW // 8) ** -0.5, 0.75, ((1, 32),), jnp.float32),
        "neighbour_modes": normal_values(seeds[2], (MODES, NSUB, IW), (IW // 8) ** -0.5, 0.75, ((1, 32),), jnp.float32),
        "face_index": draw_face_index(jax.random.fold_in(seeds[6], 71), 0),
        "neighbour_list": draw_neighbour_list(jax.random.fold_in(seeds[6], 71), 0),
        "coarse_factor": normal_values(seeds[5], (NC, NC), NC ** -0.5, 0.21875, ((0, 16), (1, 2)), jnp.float32),
    }


HIGHEST = lax.Precision.HIGHEST


def reference(multipliers, own_modes, neighbour_modes, face_index, neighbour_list, coarse_factor):
    masked_modes = []
    for which_face in range(NFACE):
        masked_modes.append(neighbour_modes * (face_index == which_face).astype(jnp.float32)[None])
    coarse = jnp.einsum('ksm,rsm->krs', own_modes, multipliers, precision=HIGHEST)
    face_parts = []
    for which_face in range(NFACE):
        face_parts.append(jnp.einsum('ksm,rsm->krs', masked_modes[which_face], multipliers, precision=HIGHEST))
    face_terms = jnp.stack(face_parts, axis=3)
    flattened = face_terms.reshape(MODES, NRHS, NSUB * NFACE).transpose(2, 0, 1)
    targets = neighbour_list.reshape(NSUB * NFACE)
    incoming = jax.ops.segment_sum(flattened, targets, num_segments=NSUB)
    coarse = coarse + incoming.transpose(1, 2, 0)
    right_side = coarse.transpose(2, 0, 1).reshape(NSUB * MODES, NRHS)
    halfway = jnp.einsum('cp,cr->pr', coarse_factor, right_side, precision=HIGHEST)
    amplitudes = jnp.dot(coarse_factor, halfway, precision=HIGHEST, preferred_element_type=jnp.float32)
    amplitudes = amplitudes.reshape(NSUB, MODES, NRHS).transpose(1, 2, 0)
    applied = jnp.einsum('ksm,krs->rsm', own_modes, amplitudes, precision=HIGHEST)
    for which_face in range(NFACE):
        across = amplitudes[:, :, neighbour_list[:, which_face]]
        applied = applied + jnp.einsum('ksm,krs->rsm', masked_modes[which_face], across, precision=HIGHEST)
    return multipliers - applied
```

```python
import jax
import jax.numpy as jnp
from jax import lax
from jax.sharding import PartitionSpec as P

MODES = 6
NFACE = 6
COL_LEN = 2
NDIR = 6
NBLOCK = 4

HIGHEST = lax.Precision.HIGHEST


def all_sum(value, axis):
    peers = lax.axis_size(axis)
    if peers & (peers - 1):
        return lax.psum(value, axis)
    step = 1
    while step < peers:
        value = value + lax.ppermute(value, axis, [(i, i ^ step) for i in range(peers)])
        step *= 2
    return value


def body(multipliers, own_modes, neighbour_modes, face_index, neighbour_list, coarse_factor):
    width_rhs, local_subs, _ = multipliers.shape
    crs_size = lax.axis_size("crs")
    sub_size = lax.axis_size("sub")
    crs_rank = lax.axis_index("crs")
    sub_rank = lax.axis_index("sub")
    group_subs = local_subs * crs_size
    row_len = sub_size // COL_LEN
    first_sub = (sub_rank * crs_size + crs_rank) * local_subs

    def ring(i, by):
        return i // row_len * row_len + (i + by) % row_len

    def fetched(source):
        return lax.ppermute(coarse_factor, "sub", [(source(i), i) for i in range(sub_size)])

    factors = [
        coarse_factor,
        fetched(lambda i: (i + row_len) % sub_size),
        fetched(lambda i: ring(i, 1)),
        fetched(lambda i: ring(i, -1)),
    ]

    local_ids = first_sub + lax.iota(jnp.int32, local_subs)
    first = local_ids // (row_len * group_subs)
    second = local_ids // group_subs % row_len
    third = local_ids % group_subs

    def place(a, b, c):
        return (a * row_len + b) * group_subs + c

    across = [
        place((first + 1) % COL_LEN, second, third),
        place(first, (second + 1) % row_len, third),
        place(first, (second + row_len - 1) % row_len, third),
        place(first, second, (third + 1) % group_subs),
        place(first, second, (third + group_subs - 1) % group_subs),
    ]
    local_nbrs = lax.dynamic_slice_in_dim(neighbour_list, first_sub, local_subs, 0)
    face_dir = jnp.zeros_like(local_nbrs)
    for which in range(NDIR - 2, -1, -1):
        face_dir = jnp.where(local_nbrs == across[which][:, None], which + 1, face_dir)
    point_dir = jnp.zeros_like(face_index)
    for which_face in range(NFACE):
        point_dir = jnp.where(
            face_index == which_face, face_dir[:, which_face : which_face + 1], point_dir
        )
    rows = [own_modes]
    for which in range(1, NDIR):
        rows.append(jnp.where((point_dir == which)[None], neighbour_modes, 0.0))
    rows = jnp.stack(rows)
    sums = jnp.einsum("dksm,rsm->rsdk", rows, multipliers, precision=HIGHEST)

    blocks = jnp.array([0, 1, 2, 3, 0, 0], jnp.int32)
    moves = jnp.array([0, 0, 0, 0, 1, group_subs - 1], jnp.int32)
    target_sub = (third[:, None] + moves[None]) % group_subs
    target = (blocks[None] * group_subs + target_sub)[:, :, None] * MODES + lax.iota(jnp.int32, MODES)
    wide = NBLOCK * group_subs * MODES
    chosen = (target.reshape(-1, 1) == lax.iota(jnp.int32, wide)[None]).astype(jnp.float32)

    coarse = jnp.dot(sums.reshape(width_rhs, -1), chosen, precision=HIGHEST)
    coarse = all_sum(coarse, "crs").reshape(width_rhs, NBLOCK, group_subs * MODES)
    panel = 0.0
    for which in range(NBLOCK):
        panel = panel + jnp.dot(coarse[:, which], factors[which], precision=HIGHEST)
    panel = all_sum(panel, "sub")
    amps = jnp.concatenate(
        [jnp.einsum("rp,cp->rc", panel, f, precision=HIGHEST) for f in factors], axis=1
    )
    amps = all_sum(amps, "crs")
    near = jnp.einsum("rw,nw->rn", amps, chosen, precision=HIGHEST)
    near = near.reshape(width_rhs, local_subs, NDIR, MODES)
    return multipliers - jnp.einsum("rsdk,dksm->rsm", near, rows, precision=HIGHEST)


def solution(mesh):
    placed = (
        P(None, ("sub", "crs"), None),
        P(None, ("sub", "crs"), None),
        P(None, ("sub", "crs"), None),
        P(("sub", "crs"), None),
        P(),
        P("sub", "crs"),
    )
    return jax.shard_map(
        body, mesh=mesh, in_specs=placed, out_specs=P(None, ("sub", "crs"), None), check_vma=False
    )
```

```python
import jax
import jax.numpy as jnp
from jax import lax
from jax.sharding import PartitionSpec as P


MODES = 6
NFACE = 6
COL_LEN = 2
NDIR = 6
NBLOCK = 4

HIGHEST = lax.Precision.HIGHEST


def all_sum(value, axis):
    peers = lax.axis_size(axis)
    if peers & (peers - 1):
        return lax.psum(value, axis)
    step = 1
    while step < peers:
        value = value + lax.ppermute(value, axis, [(i, i ^ step) for i in range(peers)])
        step *= 2
    return value


def parity(i):
    return bin(i).count("1") % 2


def crossed_sum(value):
    peers = lax.axis_size("sub")
    step = 1
    while step < peers:
        pairs = [(2 * i + c, 2 * (i ^ step) + 1 - c) for i in range(peers) for c in range(2)]
        value = value + lax.ppermute(value, ("sub", "crs"), pairs)
        step *= 2
    return value


def body(multipliers, own_modes, neighbour_modes, face_index, neighbour_list, coarse_factor):
    width_rhs, local_subs, _ = multipliers.shape
    crs_size = lax.axis_size("crs")
    sub_size = lax.axis_size("sub")
    crs_rank = lax.axis_index("crs")
    sub_rank = lax.axis_index("sub")
    group_subs = local_subs * crs_size
    row_len = sub_size // COL_LEN
    first_sub = (sub_rank * crs_size + crs_rank) * local_subs

    crossed = crs_size == 2 and sub_size & (sub_size - 1) == 0

    def ring(i, by):
        return i // row_len * row_len + (i + by) % row_len

    def fetched(source):
        pairs = []
        for i in range(sub_size):
            for c in range(crs_size):
                half = c ^ parity(i) if crossed else c
                pairs.append((source(i) * crs_size + half, i * crs_size + c))
        return lax.ppermute(coarse_factor, ("sub", "crs"), pairs)

    own_factor = coarse_factor
    if crossed:
        other = lax.ppermute(coarse_factor, "crs", [(0, 1), (1, 0)])
        own_factor = jnp.where(lax.population_count(sub_rank) % 2 == 1, other, coarse_factor)
    factors = [
        own_factor,
        fetched(lambda i: (i + row_len) % sub_size),
        fetched(lambda i: ring(i, 1)),
        fetched(lambda i: ring(i, -1)),
    ]

    local_ids = first_sub + lax.iota(jnp.int32, local_subs)
    first = local_ids // (row_len * group_subs)
    second = local_ids // group_subs % row_len
    third = local_ids % group_subs

    def place(a, b, c):
        return (a * row_len + b) * group_subs + c

    across = [
        place((first + 1) % COL_LEN, second, third),
        place(first, (second + 1) % row_len, third),
        place(first, (second + row_len - 1) % row_len, third),
        place(first, second, (third + 1) % group_subs),
        place(first, second, (third + group_subs - 1) % group_subs),
    ]
    local_nbrs = lax.dynamic_slice_in_dim(neighbour_list, first_sub, local_subs, 0)
    face_dir = jnp.zeros_like(local_nbrs)
    for which in range(NDIR - 2, -1, -1):
        face_dir = jnp.where(local_nbrs == across[which][:, None], which + 1, face_dir)
    point_dir = jnp.zeros_like(face_index)
    for which_face in range(NFACE):
        point_dir = jnp.where(
            face_index == which_face, face_dir[:, which_face : which_face + 1], point_dir
        )
    rows = [own_modes]
    for which in range(1, NDIR):
        rows.append(jnp.where((point_dir == which)[None], neighbour_modes, 0.0))
    rows = jnp.stack(rows)
    sums = jnp.einsum("dksm,rsm->rsdk", rows, multipliers, precision=HIGHEST)

    blocks = jnp.array([0, 1, 2, 3, 0, 0], jnp.int32)
    moves = jnp.array([0, 0, 0, 0, 1, group_subs - 1], jnp.int32)
    target_sub = (third[:, None] + moves[None]) % group_subs
    target = (blocks[None] * group_subs + target_sub)[:, :, None] * MODES + lax.iota(jnp.int32, MODES)
    wide = NBLOCK * group_subs * MODES
    chosen = (target.reshape(-1, 1) == lax.iota(jnp.int32, wide)[None]).astype(jnp.float32)

    coarse = jnp.dot(sums.reshape(width_rhs, -1), chosen, precision=HIGHEST)
    coarse = all_sum(coarse, "crs").reshape(width_rhs, NBLOCK, group_subs * MODES)
    panel = 0.0
    for which in range(NBLOCK):
        panel = panel + jnp.dot(coarse[:, which], factors[which], precision=HIGHEST)
    panel = crossed_sum(panel) if crossed else all_sum(panel, "sub")
    amps = jnp.concatenate(
        [jnp.einsum("rp,cp->rc", panel, f, precision=HIGHEST) for f in factors], axis=1
    )
    amps = all_sum(amps, "crs")
    near = jnp.einsum("rw,nw->rn", amps, chosen, precision=HIGHEST)
    near = near.reshape(width_rhs, local_subs, NDIR, MODES)
    return multipliers - jnp.einsum("rsdk,dksm->rsm", near, rows, precision=HIGHEST)


def solution(mesh):
    placed = (
        P(None, ("sub", "crs"), None),
        P(None, ("sub", "crs"), None),
        P(None, ("sub", "crs"), None),
        P(("sub", "crs"), None),
        P(),
        P("sub", "crs"),
    )
    return jax.shard_map(
        body, mesh=mesh, in_specs=placed, out_specs=P(None, ("sub", "crs"), None), check_vma=False
    )
```

```python
import jax
import jax.numpy as jnp
from jax import lax
from jax.experimental import pallas as pl
from jax.experimental.pallas import tpu as pltpu
from jax.sharding import PartitionSpec as P


MODES = 6
NFACE = 6
COL_LEN = 2
NDIR = 6
NBLOCK = 4

HIGHEST = lax.Precision.HIGHEST


def all_sum(value, axis):
    peers = lax.axis_size(axis)
    if peers & (peers - 1):
        return lax.psum(value, axis)
    step = 1
    while step < peers:
        value = value + lax.ppermute(value, axis, [(i, i ^ step) for i in range(peers)])
        step *= 2
    return value


def parity(i):
    return bin(i).count("1") % 2


def crossed_sum(value):
    peers = lax.axis_size("sub")
    step = 1
    while step < peers:
        pairs = [(2 * i + c, 2 * (i ^ step) + 1 - c) for i in range(peers) for c in range(2)]
        value = value + lax.ppermute(value, ("sub", "crs"), pairs)
        step *= 2
    return value


def split_rows(face_dir, own, neighbour, face, rows):
    for s in range(rows.shape[0]):
        points = face[s : s + 1, :]
        toward = jnp.zeros_like(points)
        for f in range(NFACE):
            toward = jnp.where(points == f, face_dir[s, f], toward)
        near = neighbour[:, s, :]
        rows[s, 0] = own[:, s, :]
        for d in range(1, NDIR):
            rows[s, d] = jnp.where(toward == d, near, 0.0)


def body(multipliers, own_modes, neighbour_modes, face_index, neighbour_list, coarse_factor):
    width_rhs, local_subs, _ = multipliers.shape
    crs_size = lax.axis_size("crs")
    sub_size = lax.axis_size("sub")
    crs_rank = lax.axis_index("crs")
    sub_rank = lax.axis_index("sub")
    group_subs = local_subs * crs_size
    row_len = sub_size // COL_LEN
    first_sub = (sub_rank * crs_size + crs_rank) * local_subs

    crossed = crs_size == 2 and sub_size & (sub_size - 1) == 0

    def ring(i, by):
        return i // row_len * row_len + (i + by) % row_len

    def fetched(source):
        pairs = []
        for i in range(sub_size):
            for c in range(crs_size):
                half = c ^ parity(i) if crossed else c
                pairs.append((source(i) * crs_size + half, i * crs_size + c))
        return lax.ppermute(coarse_factor, ("sub", "crs"), pairs)

    own_factor = coarse_factor
    if crossed:
        other = lax.ppermute(coarse_factor, "crs", [(0, 1), (1, 0)])
        own_factor = jnp.where(lax.population_count(sub_rank) % 2 == 1, other, coarse_factor)
    factors = [
        own_factor,
        fetched(lambda i: (i + row_len) % sub_size),
        fetched(lambda i: ring(i, 1)),
        fetched(lambda i: ring(i, -1)),
    ]

    local_ids = first_sub + lax.iota(jnp.int32, local_subs)
    first = local_ids // (row_len * group_subs)
    second = local_ids // group_subs % row_len
    third = local_ids % group_subs

    def place(a, b, c):
        return (a * row_len + b) * group_subs + c

    across = [
        place((first + 1) % COL_LEN, second, third),
        place(first, (second + 1) % row_len, third),
        place(first, (second + row_len - 1) % row_len, third),
        place(first, second, (third + 1) % group_subs),
        place(first, second, (third + group_subs - 1) % group_subs),
    ]
    local_nbrs = lax.dynamic_slice_in_dim(neighbour_list, first_sub, local_subs, 0)
    face_dir = jnp.zeros_like(local_nbrs)
    for which in range(NDIR - 2, -1, -1):
        face_dir = jnp.where(local_nbrs == across[which][:, None], which + 1, face_dir)
    rows = pl.pallas_call(
        split_rows,
        out_shape=pltpu.VMEM((local_subs, NDIR, MODES, face_index.shape[1]), jnp.float32),
        in_specs=[
            pl.BlockSpec(memory_space=pltpu.SMEM),
            pl.BlockSpec(memory_space=pltpu.VMEM),
            pl.BlockSpec(memory_space=pltpu.VMEM),
            pl.BlockSpec(memory_space=pltpu.VMEM),
        ],
        out_specs=pl.BlockSpec(memory_space=pltpu.VMEM),
        name="split_rows",
    )(face_dir, own_modes, neighbour_modes, face_index)
    sums = jnp.einsum("sdkm,rsm->rsdk", rows, multipliers, precision=HIGHEST)

    ways = lax.iota(jnp.int32, NDIR)
    blocks = jnp.where(ways < NBLOCK, ways, 0)
    moves = jnp.where(ways == 4, 1, jnp.where(ways == 5, group_subs - 1, 0))
    target_sub = (third[:, None] + moves[None]) % group_subs
    target = (blocks[None] * group_subs + target_sub)[:, :, None] * MODES + lax.iota(jnp.int32, MODES)
    wide = NBLOCK * group_subs * MODES
    chosen = (target.reshape(-1, 1) == lax.iota(jnp.int32, wide)[None]).astype(jnp.float32)

    coarse = jnp.dot(sums.reshape(width_rhs, -1), chosen, precision=HIGHEST)
    coarse = all_sum(coarse, "crs").reshape(width_rhs, NBLOCK, group_subs * MODES)
    panel = 0.0
    for which in range(NBLOCK):
        panel = panel + jnp.dot(coarse[:, which], factors[which], precision=HIGHEST)
    panel = crossed_sum(panel) if crossed else all_sum(panel, "sub")
    amps = jnp.concatenate(
        [jnp.einsum("rp,cp->rc", panel, f, precision=HIGHEST) for f in factors], axis=1
    )
    amps = all_sum(amps, "crs")
    near = jnp.einsum("rw,nw->rn", amps, chosen, precision=HIGHEST)
    near = near.reshape(width_rhs, local_subs, NDIR, MODES)
    return multipliers - jnp.einsum("rsdk,sdkm->rsm", near, rows, precision=HIGHEST)


def solution(mesh):
    placed = (
        P(None, ("sub", "crs"), None),
        P(None, ("sub", "crs"), None),
        P(None, ("sub", "crs"), None),
        P(("sub", "crs"), None),
        P(),
        P("sub", "crs"),
    )
    return jax.shard_map(
        body, mesh=mesh, in_specs=placed, out_specs=P(None, ("sub", "crs"), None), check_vma=False
    )
```
